1024 devices in a mesh: zone: 16 (over y, core), grp: 64 (over z, x).
Axes of the slice: x: 4, y: 8, z: 16, core: 2. Of those that a mesh axis runs over, the one named last changes fastest.
Arguments:
- positions: float32 [3, 2097152], P(None, ('zone', 'grp')), may hold values from 0 to 1
- masses: float32 [2097152], P(('zone', 'grp')), may hold values from 0.0009765625 to 0.015625
- active: int32 [2097152], P(('zone', 'grp')), may hold values 0 or 1
- near_src: int32 [8192, 8], P(('zone', 'grp')), may hold values from 0 to 511, as said below
- multipoles: bfloat16 [81, 32768], P(None, ('zone', 'grp')), may hold values from -6 to 6
- far_src: int32 [32768, 189], P(('zone', 'grp')), may hold values from 0 to 95
- far_class: int32 [32768, 189], P(('zone', 'grp')), may hold values from 0 to 315
- m2l_ops: bfloat16 [81, 25596], replicated, may hold values from -0.046875 to 0.046875
Outputs:
- accel: float32 [3, 2097152], P(None, ('zone', 'grp'))
- local_coeffs: float32 [81, 32768], P(None, ('zone', 'grp'))
The draws below stay inside these ranges and needn't reach their ends.
Inputs may be any that keep to these rules, and one draw needn't show every extreme that they name: `near_src`: of the 64 entries of one device's rows, at most 2 name leaves held by any one device of the zone (leaves s * 8 to s * 8 + 7 for device s), and exactly 2 name those of some device.
All inputs are finite; a program needn't handle non-finite values. No bound on the sum of `active` on one device may be relied on, other than what follows from the above.
Results may differ from the reference program's by a relative error of at most 0.0021.
Values may be sent and summed in bfloat16 or wider, within the bound.
A program may use at most 32 MiB of HBM per device.

```python
import math
import jax
import jax.numpy as jnp
from jax import lax

LEAF = 256
MC = 81
CLASSES = 316
FAR = 189
NEAR = 8
LEAF_DEV = 8
CELL_DEV = 32
CAP = 2
PARTICLES = 2097152
CELLS = 32768
N_ZONE = 16
N_GRP = 64
DEVICES = 1024


def draw_near_src(key, part):
    total = N_GRP * CAP
    pairs = LEAF_DEV * NEAR

    def one_device(index):
        subkey = jax.random.fold_in(jax.random.fold_in(key, 7919), index)
        first, second, third = jax.random.split(subkey, 3)
        order_perm = jax.random.permutation(first, total)
        heavy = order_perm[0] // CAP
        idents = jnp.arange(total, dtype=jnp.int32)
        position = jnp.argsort(order_perm, stable=True).astype(jnp.int32)
        score = jnp.where(idents // CAP == heavy, -1, position)
        chosen = jnp.argsort(score, stable=True)[:pairs].astype(jnp.int32)
        owners = (chosen // CAP)[jax.random.permutation(second, pairs)]
        locals_drawn = jax.random.randint(third, (pairs,), 0, LEAF_DEV, dtype=jnp.int32)
        return (owners * LEAF_DEV + locals_drawn).reshape(LEAF_DEV, NEAR)
    blocks = jax.vmap(one_device)(jnp.arange(DEVICES, dtype=jnp.int32))
    return blocks.reshape(DEVICES * LEAF_DEV, NEAR).astype(jnp.int32)


def with_ends(entries, rng, least, top_value):
    longest = entries.shape.index(max(entries.shape))
    spots = []
    for shift in (0, 1):
        where = [jax.random.randint(jax.random.fold_in(rng, axis), (), 0, length) for axis, length in enumerate(entries.shape)]
        where[longest] = (where[longest] + shift) % entries.shape[longest]
        spots.append(tuple(where))
    return entries.at[spots[0]].set(least).at[spots[1]].set(top_value)


def block_scale(rng, shape, cuts, smallest, largest):
    gain, own = 1.0, jax.random.fold_in(rng, 6)
    for dim, shards_of in cuts:
        heights = jnp.exp(jax.random.uniform(jax.random.fold_in(own, dim), (shards_of,), jnp.float32, smallest / len(cuts), largest / len(cuts)))
        gain = gain * jnp.repeat(heights, shape[dim] // shards_of).reshape([-1 if axis == dim else 1 for axis in range(len(shape))])
    return gain


def normal_values(stream_key, extent, deviation, limit, cuts=(), kind=jnp.bfloat16):
    result = deviation * jax.random.normal(stream_key, extent, jnp.float32)
    if cuts:
        result = result * block_scale(stream_key, extent, cuts, -0.22, 0.18)
    return jnp.clip(result, -limit, limit).astype(kind)


def setup_inputs(seed: int = 0) -> dict:
    keys = jax.random.split(jax.random.key(seed), 9)
    positions = jnp.clip(1.0 * jax.random.uniform(keys[0], (3, PARTICLES), jnp.float32) ** block_scale(keys[0], (3, PARTICLES), ((1, 1024),), -0.2, 0.2), 0.0, 1.0)
    masses = jnp.clip(jnp.exp(math.log(0.015625) - 2.7725887 * jax.random.uniform(keys[1], (PARTICLES,), jnp.float32) ** block_scale(keys[1], (PARTICLES,), ((0, 1024),), -0.2, 0.2)), 0.0009765625, 0.015625)
    active = with_ends((jax.random.randint(keys[2], (PARTICLES,), 0, 2) < 1).astype(jnp.int32), jax.random.fold_in(keys[2], 1), 0, 1)
    near_src = draw_near_src(jax.random.fold_in(keys[8], 71), 0)
    multipoles = normal_values(keys[4], (MC, CELLS), 1.0, 6.0, ((1, 1024),))
    far_src = with_ends(jax.random.randint(keys[5], (CELLS, FAR), 0, 3 * CELL_DEV), jax.random.fold_in(keys[5], 1), 0, (3 * CELL_DEV) - 1).astype(jnp.int32)
    far_class = with_ends(jax.random.randint(keys[6], (CELLS, FAR), 0, CLASSES), jax.random.fold_in(keys[6], 1), 0, CLASSES - 1).astype(jnp.int32)
    m2l_ops = normal_values(keys[7], (MC, CLASSES * MC), (MC * FAR) ** -0.5, 0.046875)
    return dict(positions=positions, masses=masses, active=active, near_src=near_src, multipoles=multipoles, far_src=far_src, far_class=far_class, m2l_ops=m2l_ops)


softening = 0.0025

def pair_forces(tpos, spos, smass):
    delta = spos[:, :, None, :] - tpos[None, :, :, None]
    dist2 = lax.optimization_barrier(jnp.sum(delta * delta, axis=1)) + softening
    weight = smass[:, None, :] * lax.rsqrt(dist2) / dist2
    return lax.optimization_barrier(jnp.sum(lax.optimization_barrier(jnp.sum(delta * weight[:, None], axis=3)), axis=0))

def reference(positions, masses, active, near_src, multipoles, far_src, far_class, m2l_ops):
    zone_leaves = N_GRP * LEAF_DEV
    leafpos = positions.reshape(3, N_ZONE, zone_leaves, LEAF).transpose(1, 2, 0, 3)
    leafmass = masses.reshape(N_ZONE, zone_leaves, LEAF)
    lists = near_src.reshape(N_ZONE, zone_leaves, NEAR)

    def one_leaf(index):
        zone_id = index // zone_leaves
        leaf_id = index % zone_leaves
        chosen = lists[zone_id, leaf_id]
        return pair_forces(leafpos[zone_id, leaf_id], leafpos[zone_id][chosen], leafmass[zone_id][chosen])
    forces = lax.map(one_leaf, jnp.arange(N_ZONE * zone_leaves, dtype=jnp.int32), batch_size=16)
    accel = forces.transpose(1, 0, 2).reshape(3, -1) * active.astype(jnp.float32)
    multi = multipoles.astype(jnp.float32).reshape(MC, N_ZONE, N_GRP, CELL_DEV)
    padded = jnp.pad(multi, ((0, 0), (1, 1), (0, 0), (0, 0)))
    sources = far_src.reshape(N_ZONE, N_GRP, CELL_DEV, FAR)
    classes = far_class.reshape(N_ZONE, N_GRP, CELL_DEV, FAR)
    operators = m2l_ops.astype(jnp.float32)

    def one_device(index):
        zone_id = index // N_GRP
        group_id = index % N_GRP
        window = lax.dynamic_slice(padded, (jnp.int32(0), zone_id, group_id, jnp.int32(0)), (MC, 3, 1, CELL_DEV))
        window = window.reshape(MC, 3 * CELL_DEV)
        rows = window.T[sources[zone_id, group_id]]
        segment = jnp.arange(CELL_DEV, dtype=jnp.int32)[:, None] * CLASSES + classes[zone_id, group_id]
        sums = jax.ops.segment_sum(rows.reshape(-1, MC), segment.reshape(-1), num_segments=CELL_DEV * CLASSES)
        sums = lax.optimization_barrier(sums.astype(jnp.bfloat16)).astype(jnp.float32)
        sums = sums.reshape(CELL_DEV, CLASSES * MC)
        return jnp.dot(operators, sums.T, precision=lax.Precision.HIGHEST)
    local = lax.map(one_device, jnp.arange(N_ZONE * N_GRP, dtype=jnp.int32))
    local_coeffs = local.transpose(1, 0, 2).reshape(MC, -1)
    return (accel, local_coeffs)
```

```python
import functools
import jax
import jax.numpy as jnp
from jax import lax
from jax.experimental import pallas as pl
from jax.experimental.pallas import tpu as pltpu
from jax.sharding import PartitionSpec as P

F32, BF16, I32 = jnp.float32, jnp.bfloat16, jnp.int32
SOFT = 0.0025
NT = (((1,), (1,)), ((), ()))
NN = (((1,), (0,)), ((), ()))


def dot(a, b, dims=NN):
    return lax.dot_general(a, b, dims, preferred_element_type=F32)


def packed(x, y, z, m):
    def q(v):
        return jnp.minimum((v * 65536.0).astype(I32), 65535) - 32768

    mass = jnp.minimum((m * 4194304.0 + 0.5).astype(I32), 65535)
    return (q(x) << 16) | (q(y) & 65535), (q(z) << 16) | mass


def features(w0, w1):
    row = lax.broadcasted_iota(I32, w0.shape, 0)
    comp = jnp.where(row < 3, row, row - 3)
    w = jnp.where(comp == 2, w1, w0)
    up = jnp.where(comp == 1, 16, 0)
    high = (w << up) >> 24
    low = lax.shift_right_logical(w << (up + 8), 24)
    part = jnp.where(
        row < 3, high.astype(F32) * (1.0 / 256), low.astype(F32) * (1.0 / 65536)
    )
    swap = jnp.where(
        row < 3, low.astype(F32) * (1.0 / 65536), high.astype(F32) * (1.0 / 256)
    )
    part = jnp.where(row < 6, part, 0.0)
    swap = jnp.where(row < 6, swap, 0.0)
    px = (w0 >> 16).astype(F32) * (1.0 / 65536)
    py = ((w0 << 16) >> 16).astype(F32) * (1.0 / 65536)
    pz = (w1 >> 16).astype(F32) * (1.0 / 65536)
    mass = (w1 & 65535).astype(F32) * (1.0 / 4194304)
    norm = px * px + py * py + pz * pz
    return row, part, swap, px, py, pz, mass, norm


def three(v):
    a = v.astype(BF16).astype(F32)
    b = (v - a).astype(BF16).astype(F32)
    c = v - a - b
    return a, b, c


def source_rows(w0, w1):
    row, part, _, px, py, pz, mass, norm = features(w0, w1)
    a, b, c = three(norm)
    extra = jnp.where(row == 0, a, jnp.where(row == 1, b, jnp.where(row == 2, c, jnp.where(row < 6, 1.0, 0.0))))
    s = jnp.concatenate([part, part, extra, jnp.zeros_like(part)], axis=0).astype(BF16)
    q = row & 3
    v = mass * jnp.where(q == 0, px, jnp.where(q == 1, py, jnp.where(q == 2, pz, 1.0)))
    hi = v.astype(BF16).astype(F32)
    b = jnp.where(row < 4, hi, v - hi).astype(BF16)
    return s, b


def target_rows(w0, w1):
    row, part, swap, px, py, pz, mass, norm = features(w0, w1)
    a, b, c = three(norm + SOFT)
    extra = jnp.where(row < 3, 1.0, jnp.where(row == 3, a, jnp.where(row == 4, b, jnp.where(row == 5, c, 0.0))))
    t = jnp.concatenate([part * -2.0, swap * -2.0, extra, jnp.zeros_like(part)], axis=0)
    return t, px[0:1], py[0:1], pz[0:1]


def words(ref, leaf, width):
    w = ref[leaf]
    return (
        jnp.broadcast_to(w[0:1], (8, width)),
        jnp.broadcast_to(w[1:2], (8, width)),
    )


def near_kernel(leaves, near, width, idx_ref, table_ref, own_ref, act_ref, out_ref):
    def one_leaf(t, carry):
        tgt, px, py, pz = target_rows(*words(own_ref, t, width))
        tt = jnp.transpose(tgt).astype(BF16)
        acc = jnp.zeros((width, 8), F32)
        for s in range(near):
            leaf = idx_ref[t * near + s]
            rows, b = source_rows(*words(table_ref, leaf, width))
            d = dot(tt, rows)
            r = lax.rsqrt(d)
            w = (r * r * r).astype(BF16)
            acc = acc + dot(w, b, NT)
        f = jnp.transpose(acc)
        f = f[0:4] + f[4:8]
        m = f[3:4]
        act = act_ref[pl.ds(t, 1), :].astype(F32)
        res = jnp.concatenate([(f[0:1] - px * m), (f[1:2] - py * m), (f[2:3] - pz * m)], axis=0) * act
        out_ref[:, pl.ds(pl.multiple_of(t * width, width), width)] = res
        return carry

    lax.fori_loop(0, leaves, one_leaf, 0)


def near_call(idx, table, own, act):
    leaves, _, width = own.shape
    near = idx.shape[0] // leaves
    return pl.pallas_call(
        functools.partial(near_kernel, leaves, near, width),
        out_shape=jax.ShapeDtypeStruct((3, leaves * width), F32),
        in_specs=[pl.BlockSpec(memory_space=pltpu.SMEM)]
        + [pl.BlockSpec(memory_space=pltpu.VMEM)] * 3,
        out_specs=pl.BlockSpec(memory_space=pltpu.VMEM),
    )(idx, table, own, act)


def place(c):
    return (c & ~63) | ((c & 7) << 3) | ((c >> 3) & 7)


def m2l_kernel(cells, coeffs, classes, cpad, kpad, src_ref, cls_ref, mp_ref, ops_ref, out_ref, src_s, cls_s, r_s, g_s):
    far = src_ref.shape[1]
    src_s[...] = jnp.full(src_s.shape, -1, I32)
    cls_s[...] = jnp.full(cls_s.shape, -1, I32)
    src_s[:, 0:far] = src_ref[...]
    cls_s[:, 0:far] = place(cls_ref[...])
    rows = (coeffs + 15) // 16 * 16
    mp = jnp.concatenate([mp_ref[...].astype(F32), jnp.zeros((rows - coeffs, mp_ref.shape[1]), F32)], axis=0).astype(BF16)
    nsrc = mp.shape[1]
    r_s[...] = jnp.zeros(r_s.shape, BF16)

    def gather_cells(i, carry):
        for u in range(UR):
            t = i * UR + u
            src = src_s[pl.ds(t, 1), :]
            pick = (lax.broadcasted_iota(I32, (nsrc, kpad), 0) == src).astype(F32).astype(BF16)
            r_s[t, 0:rows, :] = dot(mp, pick).astype(BF16)
        return carry

    lax.fori_loop(0, cells // UR, gather_cells, 0)

    def one_cell(t):
        cls = cls_s[pl.ds(t, 1), :]
        hot = (lax.broadcasted_iota(I32, (cpad, kpad), 0) == cls).astype(F32).astype(BF16)
        g = dot(hot, r_s[t], NT)
        for v in range(cpad // 8):
            part = g[8 * v : 8 * v + 8]
            shift, stride = (64 * (v // 8) + v % 8) * coeffs % 128, 8 * coeffs % 128
            if shift + 7 * stride >= 128:
                part = pltpu.roll(part, shift, 1)
                shift = 0
            part = pltpu.roll(part, shift, 1, stride=stride, stride_axis=0)
            g_s[pl.ds(t + 8 * v * cells, 8, stride=cells), :] = part

    def some_cells(i, carry):
        for u in range(UG):
            one_cell(i * UG + u)
        return carry

    lax.fori_loop(0, cells // UG, some_cells, 0)
    lane = lax.broadcasted_iota(I32, (cells, 128), 1)
    tiles = (coeffs * classes + 127) // 128
    whole = coeffs * classes // 128

    def rows_of(c):
        return g_s[pl.ds(pl.multiple_of(place(c) * cells, cells), cells), :]

    def values(q):
        c = q * 128 // coeffs
        edge = (c + 1) * coeffs - q * 128
        x = jnp.where(lane < edge, rows_of(c), rows_of(jnp.minimum(c + 1, classes - 1)))
        x = jnp.where(lane < edge + coeffs, x, rows_of(jnp.minimum(c + 2, classes - 1)))
        return x.astype(BF16)

    def step(i, acc):
        for u in range(0, UF, 2):
            q = i * UF + u
            o = ops_ref[:, pl.ds(pl.multiple_of(q * 128, 256), 256)]
            acc = acc + dot(o, jnp.concatenate([values(q), values(q + 1)], axis=1), NT)
        return acc

    main = (tiles - 1) // UF
    acc = lax.fori_loop(0, main, step, jnp.zeros((coeffs, cells), F32))
    for q in range(main * UF, tiles):
        end = min(q * 128 + 128, coeffs * classes)
        o = ops_ref[:, q * 128 : end]
        x = values(jnp.int32(q))
        if end < q * 128 + 128:
            o = jnp.concatenate([o, jnp.zeros((coeffs, q * 128 + 128 - end), o.dtype)], axis=1)
            x = jnp.where(lane < end - q * 128, x.astype(F32), 0.0).astype(BF16)
        acc = acc + dot(o, x, NT)
    out_ref[...] = acc


UR, UG, UF = 4, 4, 8


def m2l_call(src, cls, mp, ops):
    cells, far = src.shape
    coeffs = mp.shape[0]
    classes = ops.shape[1] // coeffs
    cpad = (classes + 63) // 64 * 64
    kpad = (far + 127) // 128 * 128
    return pl.pallas_call(
        functools.partial(m2l_kernel, cells, coeffs, classes, cpad, kpad),
        out_shape=jax.ShapeDtypeStruct((coeffs, cells), F32),
        in_specs=[pl.BlockSpec(memory_space=pltpu.VMEM)] * 4,
        out_specs=pl.BlockSpec(memory_space=pltpu.VMEM),
        scratch_shapes=[
            pltpu.VMEM((cells, kpad), I32),
            pltpu.VMEM((cells, kpad), I32),
            pltpu.VMEM((cells, 128, kpad), BF16),
            pltpu.VMEM((cpad * cells, 128), F32),
        ],
        compiler_params=pltpu.CompilerParams(vmem_limit_bytes=48 * 1024 * 1024),
        cost_estimate=pl.CostEstimate(flops=10**10, bytes_accessed=5 * 10**6, transcendentals=0),
    )(src, cls, mp, ops)


def on_device(positions, masses, active, near_src, multipoles, far_src, far_class, m2l_ops):
    leaves, near = near_src.shape
    width = positions.shape[1] // leaves
    w0, w1 = packed(positions[0], positions[1], positions[2], masses)
    own = jnp.stack([w0.reshape(leaves, width), w1.reshape(leaves, width)], axis=1)
    table = lax.all_gather(own, "grp", axis=0, tiled=True)
    zones = lax.axis_size("zone")
    up = [(i, i + 1) for i in range(zones - 1)]
    down = [(i + 1, i) for i in range(zones - 1)]
    before = lax.ppermute(multipoles, "zone", up)
    after = lax.ppermute(multipoles, "zone", down)
    local = m2l_call(far_src, far_class, jnp.concatenate([before, multipoles, after], axis=1), m2l_ops)
    accel = near_call(near_src.reshape(-1), table, own, active.reshape(leaves, width))
    return accel, local


def solution(mesh):
    return jax.shard_map(
        on_device,
        mesh=mesh,
        in_specs=(
            P(None, ("zone", "grp")),
            P(("zone", "grp")),
            P(("zone", "grp")),
            P(("zone", "grp"), None),
            P(None, ("zone", "grp")),
            P(("zone", "grp"), None),
            P(("zone", "grp"), None),
            P(),
        ),
        out_specs=(P(None, ("zone", "grp")), P(None, ("zone", "grp"))),
        check_vma=False,
    )
```

```python
import functools
import jax
import jax.numpy as jnp
from jax import lax
from jax.experimental import pallas as pl
from jax.experimental.pallas import tpu as pltpu
from jax.sharding import PartitionSpec as P

F32, BF16, I32 = jnp.float32, jnp.bfloat16, jnp.int32
SOFT = 0.0025
NT = (((1,), (1,)), ((), ()))
NN = (((1,), (0,)), ((), ()))


def dot(a, b, dims=NN):
    return lax.dot_general(a, b, dims, preferred_element_type=F32)


def packed(x, y, z, m):
    def q(v):
        return jnp.minimum((v * 65536.0).astype(I32), 65535) - 32768

    mass = jnp.minimum((m * 4194304.0 + 0.5).astype(I32), 65535)
    return (q(x) << 16) | (q(y) & 65535), (q(z) << 16) | mass


def features(w0, w1):
    row = lax.broadcasted_iota(I32, w0.shape, 0)
    comp = jnp.where(row < 3, row, row - 3)
    w = jnp.where(comp == 2, w1, w0)
    up = jnp.where(comp == 1, 16, 0)
    high = (w << up) >> 24
    low = lax.shift_right_logical(w << (up + 8), 24)
    part = jnp.where(
        row < 3, high.astype(F32) * (1.0 / 256), low.astype(F32) * (1.0 / 65536)
    )
    swap = jnp.where(
        row < 3, low.astype(F32) * (1.0 / 65536), high.astype(F32) * (1.0 / 256)
    )
    part = jnp.where(row < 6, part, 0.0)
    swap = jnp.where(row < 6, swap, 0.0)
    px = (w0 >> 16).astype(F32) * (1.0 / 65536)
    py = ((w0 << 16) >> 16).astype(F32) * (1.0 / 65536)
    pz = (w1 >> 16).astype(F32) * (1.0 / 65536)
    mass = (w1 & 65535).astype(F32) * (1.0 / 4194304)
    norm = px * px + py * py + pz * pz
    return row, part, swap, px, py, pz, mass, norm


def three(v):
    a = v.astype(BF16).astype(F32)
    b = (v - a).astype(BF16).astype(F32)
    c = v - a - b
    return a, b, c


def source_rows(w0, w1):
    row, part, _, px, py, pz, mass, norm = features(w0, w1)
    a, b, c = three(norm)
    extra = jnp.where(row == 0, a, jnp.where(row == 1, b, jnp.where(row == 2, c, jnp.where(row < 6, 1.0, 0.0))))
    s = jnp.concatenate([part, part, extra, jnp.zeros_like(part)], axis=0).astype(BF16)
    q = row & 3
    v = mass * jnp.where(q == 0, px, jnp.where(q == 1, py, jnp.where(q == 2, pz, 1.0)))
    hi = v.astype(BF16).astype(F32)
    b = jnp.where(row < 4, hi, v - hi).astype(BF16)
    return s, b


def target_rows(w0, w1):
    row, part, swap, px, py, pz, mass, norm = features(w0, w1)
    a, b, c = three(norm + SOFT)
    extra = jnp.where(row < 3, 1.0, jnp.where(row == 3, a, jnp.where(row == 4, b, jnp.where(row == 5, c, 0.0))))
    t = jnp.concatenate([part * -2.0, swap * -2.0, extra, jnp.zeros_like(part)], axis=0)
    return t, px[0:1], py[0:1], pz[0:1]


def words(ref, leaf, width):
    w = ref[leaf]
    return (
        jnp.broadcast_to(w[0:1], (8, width)),
        jnp.broadcast_to(w[1:2], (8, width)),
    )


def place(c):
    return (c & ~63) | ((c & 7) << 3) | ((c >> 3) & 7)


def kernel(cfg, pos_h, mass_h, act_h, near_h, mp_h, src_h, cls_h, ops_h, acc_o, loc_o,
           pos_v, mass_v, act_v, idx_s, mp_v, src_v, cls_v, ops_v, table, src_s, cls_s, mp_s, r_s, g_s,
           in_sem, halo_send, halo_recv, z_send, z_recv, x_send, x_recv):
    leaves, near, width, cells, far, coeffs, classes, cpad, kpad, zones, X, Z, R = cfg
    zone, g = lax.axis_index("zone"), lax.axis_index("grp")
    z, x = g // X, g % X
    plus, minus = Z // 2, Z - 1 - Z // 2

    def grp_at(dz, dx):
        return lax.rem(z + dz + 2 * Z, Z) * X + lax.rem(x + dx + X, X)

    def zone_at(d):
        return lax.rem(zone + d + zones, zones)

    barrier = pltpu.get_barrier_semaphore()
    reach = [d for r in range(1, R + 1) for d in (r, -r)]
    if 2 * R == Z:
        reach.remove(-R)
    peers = [{"grp": grp_at(d, 0)} for d in reach] + [{"grp": grp_at(0, d)} for d in range(1, X)]
    peers += [{"zone": zone_at(1)}, {"zone": zone_at(-1)}]
    for peer in peers:
        pl.semaphore_signal(barrier, inc=1, device_id=peer, device_id_type=MESH)

    loads = [
        pltpu.make_async_copy(a, b, in_sem.at[n])
        for n, (a, b) in enumerate(
            [(pos_h, pos_v), (mass_h, mass_v), (mp_h, mp_v.at[1]), (src_h, src_v), (cls_h, cls_v), (near_h, idx_s), (act_h, act_v), (ops_h, ops_v)]
        )
    ]
    for load in loads:
        load.start()

    loads[0].wait()
    loads[1].wait()
    own = g * leaves
    lanes = mass_v.shape[1]
    per = width // lanes
    for l in range(leaves):
        at = slice(l * width, (l + 1) * width)
        mass = jnp.concatenate([mass_v[per * l + k : per * l + k + 1, :] for k in range(per)], axis=1)
        w0, w1 = packed(pos_v[0:1, at], pos_v[1:2, at], pos_v[2:3, at], mass)
        table[own + l, 0:1, :] = w0
        table[own + l, 1:2, :] = w1
    loads[2].wait()
    pl.semaphore_wait(barrier, len(peers))

    halo = [
        pltpu.make_async_remote_copy(
            src_ref=mp_v.at[1], dst_ref=mp_v.at[1 - d], send_sem=halo_send.at[n], recv_sem=halo_recv.at[n],
            device_id={"zone": zone_at(d)}, device_id_type=MESH)
        for n, d in enumerate((1, -1))
    ]

    def block(o, dx=0):
        return table.at[pl.ds(grp_at(-o, dx) * leaves, leaves)]

    def z_copy(o, d):
        n = (o + d) % Z
        return pltpu.make_async_remote_copy(
            src_ref=block(o), dst_ref=block(o), send_sem=z_send.at[n], recv_sem=z_recv.at[n],
            device_id={"grp": grp_at(d, 0)}, device_id_type=MESH)

    def x_copy(o, dx):
        n = (dx - 1) * Z + o % Z
        return pltpu.make_async_remote_copy(
            src_ref=block(o), dst_ref=block(o), send_sem=x_send.at[n], recv_sem=x_recv.at[n],
            device_id={"grp": grp_at(0, dx)}, device_id_type=MESH)

    def z_wait(o):
        n = o % Z
        pltpu.make_async_remote_copy(
            src_ref=block(o), dst_ref=block(o), send_sem=z_send.at[n], recv_sem=z_recv.at[n],
            device_id={"grp": grp_at(1, 0)}, device_id_type=MESH).wait_recv()

    def x_wait(o, dx):
        n = (dx - 1) * Z + o % Z
        pltpu.make_async_remote_copy(
            src_ref=block(o, -dx), dst_ref=block(o, -dx), send_sem=x_send.at[n], recv_sem=x_recv.at[n],
            device_id={"grp": grp_at(0, dx)}, device_id_type=MESH).wait_recv()

    dxs = [d for d in (1, 3, 2) if d < X]
    sent = []

    def send(make, *at):
        make(*at).start()
        sent.append((make, at))

    for h in halo:
        h.start()
    for d in reversed(reach):
        send(z_copy, 0, d)
    for dx in dxs:
        send(x_copy, 0, dx)

    def arrived(o):
        z_wait(o)
        if o == R:
            for d in range(plus - R, 0, -1):
                send(z_copy, o, d)
        if o == -R:
            for d in range(minus - R, 0, -1):
                send(z_copy, o, -d)
        for dx in dxs:
            send(x_copy, o, dx)

    events = {}
    groups = cells // UG
    order = [o for r in range(1, plus + 1) for o in (r, -r) if o <= plus and -o <= minus]
    for o in order:
        a = abs(o)
        where = ("g", EV_G[a]) if a in EV_G else ("f", EV_F[a])
        events.setdefault(where, []).append(o)

    def run_events(kind, i, n):
        for k in range(n):
            if (kind, k) in events:
                @pl.when(i == k)
                def _():
                    for o in events[(kind, k)]:
                        arrived(o)

    loads[3].wait()
    loads[4].wait()
    src_s[...] = jnp.full(src_s.shape, -1, I32)
    cls_s[...] = jnp.full(cls_s.shape, -1, I32)
    src_s[:, 0:far] = src_v[...]
    cls_s[:, 0:far] = place(cls_v[...])
    mp_s[...] = jnp.zeros(mp_s.shape, F32)
    for h in halo:
        h.wait_recv()
    keep = [(zone > 0).astype(F32), 1.0, (zone < zones - 1).astype(F32)]
    for d in range(3):
        mp_s[d * cells : (d + 1) * cells, 0:coeffs] = mp_v[d].astype(F32) * keep[d]
    mp = jnp.transpose(mp_s[...]).astype(BF16)
    nsrc = 3 * cells

    def gather_cells(i, carry):
        for u in range(UR):
            t = i * UR + u
            src = src_s[pl.ds(t, 1), :]
            pick = (lax.broadcasted_iota(I32, (nsrc, kpad), 0) == src).astype(F32).astype(BF16)
            r_s[t] = dot(mp, pick).astype(BF16)
        return carry

    lax.fori_loop(0, cells // UR, gather_cells, 0)

    def one_cell(t):
        cls = cls_s[pl.ds(t, 1), :]
        hot = (lax.broadcasted_iota(I32, (cpad, kpad), 0) == cls).astype(F32).astype(BF16)
        g = dot(hot, r_s[t], NT)
        for v in range(cpad // 8):
            part = g[8 * v : 8 * v + 8]
            shift, stride = (64 * (v // 8) + v % 8) * coeffs % 128, 8 * coeffs % 128
            if shift + 7 * stride >= 128:
                part = pltpu.roll(part, shift, 1)
                shift = 0
            part = pltpu.roll(part, shift, 1, stride=stride, stride_axis=0)
            g_s[pl.ds(t + 8 * v * cells, 8, stride=cells), :] = part

    def some_cells(i, carry):
        for u in range(UG):
            one_cell(i * UG + u)
        run_events("g", i, groups)
        return carry

    lax.fori_loop(0, groups, some_cells, 0)
    lane = lax.broadcasted_iota(I32, (cells, 128), 1)
    tiles = (coeffs * classes + 127) // 128
    loads[7].wait()

    def rows_of(c):
        return g_s[pl.ds(pl.multiple_of(place(c) * cells, cells), cells), :]

    def values(q):
        c = q * 128 // coeffs
        edge = (c + 1) * coeffs - q * 128
        v = jnp.where(lane < edge, rows_of(c), rows_of(jnp.minimum(c + 1, classes - 1)))
        v = jnp.where(lane < edge + coeffs, v, rows_of(jnp.minimum(c + 2, classes - 1)))
        return v.astype(BF16)

    main = (tiles - 1) // UF

    def step(i, acc):
        for u in range(0, UF, 2):
            q = i * UF + u
            o = ops_v[:, pl.ds(pl.multiple_of(q * 128, 256), 256)]
            acc = acc + dot(jnp.concatenate([values(q), values(q + 1)], axis=1), o, NT)
        run_events("f", i, main)
        return acc

    acc = lax.fori_loop(0, main, step, jnp.zeros((cells, coeffs), F32))
    for q in range(main * UF, tiles):
        end = min(q * 128 + 128, coeffs * classes)
        o = ops_v[:, q * 128 : end]
        v = values(jnp.int32(q))
        if end < q * 128 + 128:
            o = jnp.concatenate([o, jnp.zeros((coeffs, q * 128 + 128 - end), o.dtype)], axis=1)
            v = jnp.where(lane < end - q * 128, v.astype(F32), 0.0).astype(BF16)
        acc = acc + dot(v, o, NT)
    loc_o[...] = acc

    for o in [0] + order:
        for dx in dxs:
            x_wait(o, dx)
    loads[5].wait()
    loads[6].wait()

    def one_leaf(t, carry):
        tgt, px, py, pz = target_rows(*words(table, own + t, width))
        tt = jnp.transpose(tgt).astype(BF16)
        acc = jnp.zeros((width, 8), F32)
        for s in range(near):
            rows, b = source_rows(*words(table, idx_s[t, s], width))
            d = dot(tt, rows)
            r = lax.rsqrt(d)
            w = (r * r * r).astype(BF16)
            acc = acc + dot(w, b, NT)
        f = jnp.transpose(acc)
        f = f[0:4] + f[4:8]
        m = f[3:4]
        on = jnp.concatenate([act_v[pl.ds(per * t + k, 1), :] for k in range(per)], axis=1).astype(F32)
        res = jnp.concatenate([(f[0:1] - px * m), (f[1:2] - py * m), (f[2:3] - pz * m)], axis=0) * on
        acc_o[:, pl.ds(pl.multiple_of(t * width, width), width)] = res
        return carry

    lax.fori_loop(0, leaves, one_leaf, 0)
    for make, at in sent:
        make(*at).wait_send()
    for h in halo:
        h.wait_send()


UR, UG, UF = 4, 4, 8
EV_G = {1: 0, 2: 0, 3: 1, 4: 2, 5: 7}
EV_F = {6: 3, 7: 6, 8: 9}
MESH = pl.DeviceIdType.MESH
X_CHIPS = 4
REACH = 4


def on_device(positions, masses, active, near_src, multipoles, far_src, far_class, m2l_ops):
    leaves, near = near_src.shape
    particles = positions.shape[1]
    width = particles // leaves
    cells, far = far_src.shape
    coeffs = multipoles.shape[0]
    classes = m2l_ops.shape[1] // coeffs
    cpad = (classes + 63) // 64 * 64
    kpad = (far + 127) // 128 * 128
    zones, groups = lax.axis_size("zone"), lax.axis_size("grp")
    Z = groups // X_CHIPS
    cfg = (leaves, near, width, cells, far, coeffs, classes, cpad, kpad, zones, X_CHIPS, Z, REACH)
    accel, local = pl.pallas_call(
        functools.partial(kernel, cfg),
        out_shape=(jax.ShapeDtypeStruct((3, particles), F32), jax.ShapeDtypeStruct((cells, coeffs), F32)),
        in_specs=[pl.BlockSpec(memory_space=pl.ANY)] * 8,
        out_specs=(pl.BlockSpec(memory_space=pltpu.VMEM),) * 2,
        scratch_shapes=[
            pltpu.VMEM((3, particles), F32),
            pltpu.VMEM((particles // 128, 128), F32),
            pltpu.VMEM((particles // 128, 128), I32),
            pltpu.SMEM((leaves, near), I32),
            pltpu.VMEM((3, cells, coeffs), BF16),
            pltpu.VMEM((cells, far), I32),
            pltpu.VMEM((cells, far), I32),
            pltpu.VMEM(m2l_ops.shape, BF16),
            pltpu.VMEM((groups * leaves, 2, width), I32),
            pltpu.VMEM((cells, kpad), I32),
            pltpu.VMEM((cells, kpad), I32),
            pltpu.VMEM((3 * cells, 128), F32),
            pltpu.VMEM((cells, 128, kpad), BF16),
            pltpu.VMEM((cpad * cells, 128), F32),
            pltpu.SemaphoreType.DMA((8,)),
            pltpu.SemaphoreType.DMA((2,)),
            pltpu.SemaphoreType.DMA((2,)),
            pltpu.SemaphoreType.DMA((Z,)),
            pltpu.SemaphoreType.DMA((Z,)),
            pltpu.SemaphoreType.DMA(((X_CHIPS - 1) * Z,)),
            pltpu.SemaphoreType.DMA(((X_CHIPS - 1) * Z,)),
        ],
        compiler_params=pltpu.CompilerParams(
            collective_id=0, has_side_effects=True, vmem_limit_bytes=67043328),
    )(positions, masses.reshape(-1, 128), active.reshape(-1, 128), near_src, multipoles.T, far_src, far_class, m2l_ops)
    return accel, local.T


def solution(mesh):
    return jax.shard_map(
        on_device,
        mesh=mesh,
        in_specs=(
            P(None, ("zone", "grp")),
            P(("zone", "grp")),
            P(("zone", "grp")),
            P(("zone", "grp"), None),
            P(None, ("zone", "grp")),
            P(("zone", "grp"), None),
            P(("zone", "grp"), None),
            P(),
        ),
        out_specs=(P(None, ("zone", "grp")), P(None, ("zone", "grp"))),
        check_vma=False,
    )
```

```python
import functools
import jax
import jax.numpy as jnp
from jax import lax
from jax.experimental import pallas as pl
from jax.experimental.pallas import tpu as pltpu
from jax.sharding import PartitionSpec as P

F32, BF16, I32 = jnp.float32, jnp.bfloat16, jnp.int32
SOFT = 0.0025
NT = (((1,), (1,)), ((), ()))
NN = (((1,), (0,)), ((), ()))


def dot(a, b, dims=NN):
    return lax.dot_general(a, b, dims, preferred_element_type=F32)


def packed(x, y, z, m):
    def q(v):
        return jnp.minimum((v * 65536.0).astype(I32), 65535) - 32768

    mass = jnp.minimum((m * 4194304.0 + 0.5).astype(I32), 65535)
    return (q(x) << 16) | (q(y) & 65535), (q(z) << 16) | mass


def features(w0, w1):
    row = lax.broadcasted_iota(I32, w0.shape, 0)
    comp = jnp.where(row < 3, row, row - 3)
    w = jnp.where(comp == 2, w1, w0)
    up = jnp.where(comp == 1, 16, 0)
    high = (w << up) >> 24
    low = lax.shift_right_logical(w << (up + 8), 24)
    part = jnp.where(
        row < 3, high.astype(F32) * (1.0 / 256), low.astype(F32) * (1.0 / 65536)
    )
    swap = jnp.where(
        row < 3, low.astype(F32) * (1.0 / 65536), high.astype(F32) * (1.0 / 256)
    )
    part = jnp.where(row < 6, part, 0.0)
    swap = jnp.where(row < 6, swap, 0.0)
    px = (w0 >> 16).astype(F32) * (1.0 / 65536)
    py = ((w0 << 16) >> 16).astype(F32) * (1.0 / 65536)
    pz = (w1 >> 16).astype(F32) * (1.0 / 65536)
    mass = (w1 & 65535).astype(F32) * (1.0 / 4194304)
    norm = px * px + py * py + pz * pz
    return row, part, swap, px, py, pz, mass, norm


def three(v):
    a = v.astype(BF16).astype(F32)
    b = (v - a).astype(BF16).astype(F32)
    c = v - a - b
    return a, b, c


def source_rows(w0, w1):
    row, part, _, px, py, pz, mass, norm = features(w0, w1)
    a, b, c = three(norm)
    extra = jnp.where(row == 0, a, jnp.where(row == 1, b, jnp.where(row == 2, c, jnp.where(row < 6, 1.0, 0.0))))
    s = jnp.concatenate([part, part, extra, jnp.zeros_like(part)], axis=0).astype(BF16)
    q = row & 3
    v = mass * jnp.where(q == 0, px, jnp.where(q == 1, py, jnp.where(q == 2, pz, 1.0)))
    hi = v.astype(BF16).astype(F32)
    b = jnp.where(row < 4, hi, v - hi).astype(BF16)
    return s, b


def target_rows(w0, w1):
    row, part, swap, px, py, pz, mass, norm = features(w0, w1)
    a, b, c = three(norm + SOFT)
    extra = jnp.where(row < 3, 1.0, jnp.where(row == 3, a, jnp.where(row == 4, b, jnp.where(row == 5, c, 0.0))))
    t = jnp.concatenate([part * -2.0, swap * -2.0, extra, jnp.zeros_like(part)], axis=0)
    return t, px[0:1], py[0:1], pz[0:1]


def words(ref, leaf, width):
    w = ref[leaf]
    return (
        jnp.broadcast_to(w[0:1], (8, width)),
        jnp.broadcast_to(w[1:2], (8, width)),
    )


def place(c):
    return (c & ~63) | ((c & 7) << 3) | ((c >> 3) & 7)


def kernel(cfg, pos_h, mass_h, act_h, near_h, mp_h, src_h, cls_h, ops_h, acc_o, loc_o,
           pos_v, mass_v, act_v, idx_s, mp_v, src_v, cls_v, ops_v, table, src_s, cls_s, mp_s, r_s, g_s, t_s, p_s, s_s, b_s, f_s,
           in_sem, halo_send, halo_recv, z_send, z_recv, x_send, x_recv):
    leaves, near, width, cells, far, coeffs, classes, cpad, kpad, zones, X, Z, R = cfg
    zone, g = lax.axis_index("zone"), lax.axis_index("grp")
    z, x = g // X, g % X
    plus, minus = Z // 2, Z - 1 - Z // 2

    def grp_at(dz, dx):
        return lax.rem(z + dz + 2 * Z, Z) * X + lax.rem(x + dx + X, X)

    def zone_at(d):
        return lax.rem(zone + d + zones, zones)

    barrier = pltpu.get_barrier_semaphore()
    reach = [d for r in range(1, R + 1) for d in (r, -r)]
    if 2 * R == Z:
        reach.remove(-R)
    peers = [{"grp": grp_at(d, 0)} for d in reach] + [{"grp": grp_at(0, d)} for d in range(1, X)]
    peers += [{"zone": zone_at(1)}, {"zone": zone_at(-1)}]
    for peer in peers:
        pl.semaphore_signal(barrier, inc=1, device_id=peer, device_id_type=MESH)

    loads = [
        pltpu.make_async_copy(a, b, in_sem.at[n])
        for n, (a, b) in enumerate(
            [(pos_h, pos_v), (mass_h, mass_v), (mp_h, mp_v.at[1]), (src_h, src_v), (cls_h, cls_v), (near_h, idx_s), (act_h, act_v), (ops_h, ops_v)]
        )
    ]
    for load in loads:
        load.start()

    loads[0].wait()
    loads[1].wait()
    own = g * leaves
    lanes = mass_v.shape[1]
    per = width // lanes
    for l in range(leaves):
        at = slice(l * width, (l + 1) * width)
        mass = jnp.concatenate([mass_v[per * l + k : per * l + k + 1, :] for k in range(per)], axis=1)
        w0, w1 = packed(pos_v[0:1, at], pos_v[1:2, at], pos_v[2:3, at], mass)
        table[own + l, 0:1, :] = w0
        table[own + l, 1:2, :] = w1
    loads[2].wait()
    pl.semaphore_wait(barrier, len(peers))

    halo = [
        pltpu.make_async_remote_copy(
            src_ref=mp_v.at[1], dst_ref=mp_v.at[1 - d], send_sem=halo_send.at[n], recv_sem=halo_recv.at[n],
            device_id={"zone": zone_at(d)}, device_id_type=MESH)
        for n, d in enumerate((1, -1))
    ]

    def block(o, dx=0):
        return table.at[pl.ds(grp_at(-o, dx) * leaves, leaves)]

    def z_copy(o, d):
        n = (o + d) % Z
        return pltpu.make_async_remote_copy(
            src_ref=block(o), dst_ref=block(o), send_sem=z_send.at[n], recv_sem=z_recv.at[n],
            device_id={"grp": grp_at(d, 0)}, device_id_type=MESH)

    def x_copy(o, dx):
        n = (dx - 1) * Z + o % Z
        return pltpu.make_async_remote_copy(
            src_ref=block(o), dst_ref=block(o), send_sem=x_send.at[n], recv_sem=x_recv.at[n],
            device_id={"grp": grp_at(0, dx)}, device_id_type=MESH)

    def x_onward(o, dx):
        n = Z + o % Z
        return pltpu.make_async_remote_copy(
            src_ref=block(o, -dx), dst_ref=block(o, -dx), send_sem=x_send.at[n], recv_sem=x_recv.at[n],
            device_id={"grp": grp_at(0, dx)}, device_id_type=MESH)

    def z_wait(o):
        n = o % Z
        pltpu.make_async_remote_copy(
            src_ref=block(o), dst_ref=block(o), send_sem=z_send.at[n], recv_sem=z_recv.at[n],
            device_id={"grp": grp_at(1, 0)}, device_id_type=MESH).wait_recv()

    def x_wait(o, dx):
        n = (dx - 1) * Z + o % Z
        pltpu.make_async_remote_copy(
            src_ref=block(o, -dx), dst_ref=block(o, -dx), send_sem=x_send.at[n], recv_sem=x_recv.at[n],
            device_id={"grp": grp_at(0, dx)}, device_id_type=MESH).wait_recv()

    sent = []
    near_dx = (1, X - 1)

    def send(make, *at):
        make(*at).start()
        sent.append((make, at))

    for h in halo:
        h.start()
    for d in reversed(reach):
        send(z_copy, 0, d)
    for dx in near_dx if 0 in RELAYS else range(1, X):
        send(x_copy, 0, dx)

    def x_relay(o):
        dx = near_dx[o % 2]
        x_wait(o, dx)
        send(x_onward, o, dx)

    def arrived(o):
        z_wait(o)
        if o % R == 0:
            sign, most = (1, plus) if o > 0 else (-1, minus)
            for d in range(min(R, most - abs(o)), 0, -1):
                send(z_copy, o, sign * d)
        for dx in near_dx[::-1]:
            if dx == 1 and abs(o) not in RELAYS:
                send(x_copy, o, 2)
            send(x_copy, o, dx)

    order = [o for r in range(1, plus + 1) for o in (r, -r) if o <= plus and -o <= minus]
    events = {}
    for o in order:
        events.setdefault(EVENTS.get(abs(o), "end"), []).append((arrived, o))
    for o in [0] + order:
        if abs(o) in RELAYS:
            events.setdefault(RELAYS[abs(o)], []).append((x_relay, o))

    def run_events(key):
        for act, o in events.get(key, ()):
            act(o)

    loads[3].wait()
    loads[4].wait()
    src_s[...] = jnp.full(src_s.shape, -1, I32)
    cls_s[...] = jnp.full(cls_s.shape, -1, I32)
    src_s[:, 0:far] = src_v[...]
    cls_s[:, 0:far] = place(cls_v[...])
    mp_s[...] = jnp.zeros(mp_s.shape, F32)

    def target_features(t, carry):
        tgt, px, py, pz = target_rows(*words(table, own + t, width))
        t_s[t] = jnp.transpose(tgt).astype(BF16)
        p_s[t] = jnp.concatenate([px, py, pz], axis=0)
        return carry

    lax.fori_loop(0, leaves, target_features, 0, unroll=True)
    for h in halo:
        h.wait_recv()
    keep = [(zone > 0).astype(F32), 1.0, (zone < zones - 1).astype(F32)]
    for d in range(3):
        mp_s[d * cells : (d + 1) * cells, 0:coeffs] = mp_v[d].astype(F32) * keep[d]
    mp = jnp.transpose(mp_s[...]).astype(BF16)
    nsrc = 3 * cells

    def gather_cells(i, carry):
        for u in range(UR):
            t = i * UR + u
            src = src_s[pl.ds(t, 1), :]
            pick = (lax.broadcasted_iota(I32, (nsrc, kpad), 0) == src).astype(F32).astype(BF16)
            r_s[t] = dot(mp, pick).astype(BF16)
        return carry

    lax.fori_loop(0, cells // UR, gather_cells, 0)
    run_events("r")

    def one_cell(t):
        cls = cls_s[pl.ds(t, 1), :]
        hot = (lax.broadcasted_iota(I32, (cpad, kpad), 0) == cls).astype(F32).astype(BF16)
        g = dot(hot, r_s[t], NT)
        for v in range(cpad // 8):
            part = g[8 * v : 8 * v + 8]
            shift, stride = (64 * (v // 8) + v % 8) * coeffs % 128, 8 * coeffs % 128
            if shift + 7 * stride >= 128:
                part = pltpu.roll(part, shift, 1)
                shift = 0
            part = pltpu.roll(part, shift, 1, stride=stride, stride_axis=0)
            g_s[pl.ds(pl.multiple_of(t * cpad + 8 * v, 8), 8), :] = part

    def some_cells(i, carry):
        for u in range(UG):
            one_cell(i * UG + u)
        for k in range(cells // UG):
            if ("g", k) in events:
                @pl.when(i == k)
                def _():
                    run_events(("g", k))
        return carry

    lax.fori_loop(0, cells // UG, some_cells, 0)
    lane = lax.broadcasted_iota(I32, (cells, 128), 1)
    tiles = (coeffs * classes + 127) // 128
    loads[7].wait()

    def rows_of(c):
        return g_s[pl.ds(place(c), cells, stride=cpad), :]

    def values(q):
        c = q * 128 // coeffs
        v = rows_of(c)
        while (c + 1) * coeffs < min(q * 128 + 128, coeffs * classes):
            c += 1
            v = jnp.where(lane < c * coeffs - q * 128, v, rows_of(c))
        if (c + 1) * coeffs < q * 128 + 128:
            v = jnp.where(lane < (c + 1) * coeffs - q * 128, v, 0.0)
        return v.astype(BF16)

    acc = jnp.zeros((cells, coeffs), F32)
    for q in range(0, tiles, 2):
        run_events(("f", q // 2))
        end = min(q * 128 + 256, coeffs * classes)
        o = ops_v[:, q * 128 : end]
        if end < q * 128 + 256:
            o = jnp.concatenate([o[:, :128], o[:, 128:], jnp.zeros((coeffs, q * 128 + 256 - end), o.dtype)], axis=1)
        acc = acc + dot(jnp.concatenate([values(q), values(q + 1)], axis=1), o, NT)
    loc_o[...] = acc
    run_events("end")

    loads[5].wait()
    loads[6].wait()
    for o in [0] + order:
        for dx in range(1, X):
            if not (abs(o) in RELAYS and dx == near_dx[o % 2]):
                x_wait(o, dx)

    def source_features(i, carry):
        for u in range(US):
            n = i * US + u
            rows, b = source_rows(*words(table, idx_s[n // near, n % near], width))
            s_s[n] = rows
            b_s[n] = b
        return carry

    lax.fori_loop(0, leaves * near // US, source_features, 0)

    def some_leaves(i, carry):
        for u in range(UL):
            t = i * UL + u
            acc = jnp.zeros((width, 8), F32)
            for s in range(near):
                n = t * near + s
                r = lax.rsqrt(dot(t_s[t], s_s[n]))
                acc = acc + dot((r * r * r).astype(BF16), b_s[n], NT)
            f_s[t] = acc
        return carry

    lax.fori_loop(0, leaves // UL, some_leaves, 0)
    for t in range(leaves):
        f = jnp.transpose(f_s[t])
        f = f[0:4] + f[4:8]
        on = jnp.concatenate([act_v[per * t + k : per * t + k + 1, :] for k in range(per)], axis=1).astype(F32)
        acc_o[:, t * width : (t + 1) * width] = (f[0:3] - p_s[t] * f[3:4]) * on
    for make, at in sent:
        make(*at).wait_send()
    for h in halo:
        h.wait_send()


UR, UG, US, UL = 16, 8, 8, 4
EVENTS = {1: ("g", 0), 2: ("g", 0), 3: ("g", 0), 4: ("f", 45), 5: ("f", 45), 6: ("f", 45)}
RELAYS = {}
MESH = pl.DeviceIdType.MESH
X_CHIPS = 4
REACH = 3


def on_device(positions, masses, active, near_src, multipoles, far_src, far_class, m2l_ops):
    leaves, near = near_src.shape
    particles = positions.shape[1]
    width = particles // leaves
    cells, far = far_src.shape
    coeffs = multipoles.shape[0]
    classes = m2l_ops.shape[1] // coeffs
    cpad = (classes + 63) // 64 * 64
    kpad = (far + 127) // 128 * 128
    zones, groups = lax.axis_size("zone"), lax.axis_size("grp")
    Z = groups // X_CHIPS
    cfg = (leaves, near, width, cells, far, coeffs, classes, cpad, kpad, zones, X_CHIPS, Z, REACH)
    accel, local = pl.pallas_call(
        functools.partial(kernel, cfg),
        out_shape=(jax.ShapeDtypeStruct((3, particles), F32), jax.ShapeDtypeStruct((cells, coeffs), F32)),
        in_specs=[pl.BlockSpec(memory_space=pl.ANY)] * 8,
        out_specs=(pl.BlockSpec(memory_space=pltpu.VMEM),) * 2,
        scratch_shapes=[
            pltpu.VMEM((3, particles), F32),
            pltpu.VMEM((particles // 128, 128), F32),
            pltpu.VMEM((particles // 128, 128), I32),
            pltpu.SMEM((leaves, near), I32),
            pltpu.VMEM((3, cells, coeffs), BF16),
            pltpu.VMEM((cells, far), I32),
            pltpu.VMEM((cells, far), I32),
            pltpu.VMEM(m2l_ops.shape, BF16),
            pltpu.VMEM((groups * leaves, 2, width), I32),
            pltpu.VMEM((cells, kpad), I32),
            pltpu.VMEM((cells, kpad), I32),
            pltpu.VMEM((3 * cells, 128), F32),
            pltpu.VMEM((cells, 128, kpad), BF16),
            pltpu.VMEM((cpad * cells, 128), F32),
            pltpu.VMEM((leaves, width, 32), BF16),
            pltpu.VMEM((leaves, 3, width), F32),
            pltpu.VMEM((leaves * near, 32, width), BF16),
            pltpu.VMEM((leaves * near, 8, width), BF16),
            pltpu.VMEM((leaves, width, 8), F32),
            pltpu.SemaphoreType.DMA((8,)),
            pltpu.SemaphoreType.DMA((2,)),
            pltpu.SemaphoreType.DMA((2,)),
            pltpu.SemaphoreType.DMA((Z,)),
            pltpu.SemaphoreType.DMA((Z,)),
            pltpu.SemaphoreType.DMA(((X_CHIPS - 1) * Z,)),
            pltpu.SemaphoreType.DMA(((X_CHIPS - 1) * Z,)),
        ],
        compiler_params=pltpu.CompilerParams(
            collective_id=0, has_side_effects=True, vmem_limit_bytes=67043328),
    )(positions, masses.reshape(-1, 128), active.reshape(-1, 128), near_src, multipoles.T, far_src, far_class, m2l_ops)
    accel, local = pl.pallas_call(
        hand_over,
        out_shape=(jax.ShapeDtypeStruct(accel.shape, F32), jax.ShapeDtypeStruct(local.shape, F32)),
        in_specs=[pl.BlockSpec(memory_space=pl.ANY)] * 2,
        out_specs=(pl.BlockSpec(memory_space=pl.ANY),) * 2,
        scratch_shapes=[pltpu.VMEM(accel.shape, F32), pltpu.VMEM(local.shape, F32), pltpu.SemaphoreType.DMA((4,))],
    )(accel, local)
    return accel, local.T


def hand_over(a_in, b_in, a_out, b_out, a_v, b_v, sem):
    copies = [
        pltpu.make_async_copy(x, y, sem.at[n])
        for n, (x, y) in enumerate([(a_in, a_v), (b_in, b_v), (a_v, a_out), (b_v, b_out)])
    ]
    copies[0].start()
    copies[1].start()
    copies[1].wait()
    copies[3].start()
    copies[0].wait()
    copies[2].start()
    copies[2].wait()
    copies[3].wait()


def solution(mesh):
    return jax.shard_map(
        on_device,
        mesh=mesh,
        in_specs=(
            P(None, ("zone", "grp")),
            P(("zone", "grp")),
            P(("zone", "grp")),
            P(("zone", "grp"), None),
            P(None, ("zone", "grp")),
            P(("zone", "grp"), None),
            P(("zone", "grp"), None),
            P(),
        ),
        out_specs=(P(None, ("zone", "grp")), P(None, ("zone", "grp"))),
        check_vma=False,
    )
```

```python
import functools
import jax
import jax.numpy as jnp
from jax import lax
from jax.experimental import pallas as pl
from jax.experimental.pallas import tpu as pltpu
from jax.sharding import PartitionSpec as P

F32, BF16, I32 = jnp.float32, jnp.bfloat16, jnp.int32
SOFT = 0.0025
NT = (((1,), (1,)), ((), ()))
NN = (((1,), (0,)), ((), ()))


def dot(a, b, dims=NN):
    return lax.dot_general(a, b, dims, preferred_element_type=F32)


def packed(x, y, z, m):
    def q(v):
        return jnp.minimum((v * 65536.0).astype(I32), 65535) - 32768

    mass = jnp.minimum((m * 4194304.0 + 0.5).astype(I32), 65535)
    return (q(x) << 16) | (q(y) & 65535), (q(z) << 16) | mass


def features(w0, w1):
    row = lax.broadcasted_iota(I32, w0.shape, 0)
    comp = jnp.where(row < 3, row, row - 3)
    w = jnp.where(comp == 2, w1, w0)
    up = jnp.where(comp == 1, 16, 0)
    high = (w << up) >> 24
    low = lax.shift_right_logical(w << (up + 8), 24)
    part = jnp.where(
        row < 3, high.astype(F32) * (1.0 / 256), low.astype(F32) * (1.0 / 65536)
    )
    swap = jnp.where(
        row < 3, low.astype(F32) * (1.0 / 65536), high.astype(F32) * (1.0 / 256)
    )
    part = jnp.where(row < 6, part, 0.0)
    swap = jnp.where(row < 6, swap, 0.0)
    px = (w0 >> 16).astype(F32) * (1.0 / 65536)
    py = ((w0 << 16) >> 16).astype(F32) * (1.0 / 65536)
    pz = (w1 >> 16).astype(F32) * (1.0 / 65536)
    mass = (w1 & 65535).astype(F32) * (1.0 / 4194304)
    norm = px * px + py * py + pz * pz
    return row, part, swap, px, py, pz, mass, norm


def three(v):
    a = v.astype(BF16).astype(F32)
    b = (v - a).astype(BF16).astype(F32)
    c = v - a - b
    return a, b, c


def source_rows(w0, w1):
    row, part, _, px, py, pz, mass, norm = features(w0, w1)
    a, b, c = three(norm)
    extra = jnp.where(row == 0, a, jnp.where(row == 1, b, jnp.where(row == 2, c, jnp.where(row < 6, 1.0, 0.0))))
    s = jnp.concatenate([part, part, extra, jnp.zeros_like(part)], axis=0).astype(BF16)
    q = row & 3
    v = mass * jnp.where(q == 0, px, jnp.where(q == 1, py, jnp.where(q == 2, pz, 1.0)))
    hi = v.astype(BF16).astype(F32)
    b = jnp.where(row < 4, hi, v - hi).astype(BF16)
    return s, b


def target_rows(w0, w1):
    row, part, swap, px, py, pz, mass, norm = features(w0, w1)
    a, b, c = three(norm + SOFT)
    extra = jnp.where(row < 3, 1.0, jnp.where(row == 3, a, jnp.where(row == 4, b, jnp.where(row == 5, c, 0.0))))
    t = jnp.concatenate([part * -2.0, swap * -2.0, extra, jnp.zeros_like(part)], axis=0)
    return t, px[0:1], py[0:1], pz[0:1]


def words(ref, leaf, width):
    w = ref[leaf]
    return (
        jnp.broadcast_to(w[0:1], (8, width)),
        jnp.broadcast_to(w[1:2], (8, width)),
    )


def place(c):
    return (c & ~63) | ((c & 7) << 3) | ((c >> 3) & 7)


def kernel(cfg, pos_h, mass_h, act_h, near_h, mp_h, src_h, cls_h, ops_h, acc_o, loc_o,
           pos_v, mass_v, act_v, idx_s, mp_v, src_v, cls_v, ops_v, table, src_s, cls_s, mp_s, r_s, g_s, t_s, p_s, s_s, b_s, f_s,
           in_sem, halo_send, halo_recv, z_send, z_recv, x_send, x_recv):
    leaves, near, width, cells, far, coeffs, classes, cpad, kpad, zones, X, Z, R = cfg
    zone, g = lax.axis_index("zone"), lax.axis_index("grp")
    z, x = g // X, g % X
    plus, minus = Z // 2, Z - 1 - Z // 2

    def grp_at(dz, dx):
        return lax.rem(z + dz + 2 * Z, Z) * X + lax.rem(x + dx + X, X)

    def zone_at(d):
        return lax.rem(zone + d + zones, zones)

    barrier = pltpu.get_barrier_semaphore()
    reach = [d for r in range(1, R + 1) for d in (r, -r)]
    if 2 * R == Z:
        reach.remove(-R)
    peers = [{"grp": grp_at(d, 0)} for d in reach] + [{"grp": grp_at(0, d)} for d in range(1, X)]
    peers += [{"zone": zone_at(1)}, {"zone": zone_at(-1)}]
    for peer in peers:
        pl.semaphore_signal(barrier, inc=1, device_id=peer, device_id_type=MESH)

    loads = [
        pltpu.make_async_copy(a, b, in_sem.at[n])
        for n, (a, b) in enumerate(
            [(pos_h, pos_v), (mass_h, mass_v), (mp_h, mp_v.at[1]), (src_h, src_v), (cls_h, cls_v), (near_h, idx_s), (act_h, act_v), (ops_h, ops_v)]
        )
    ]
    for load in loads:
        load.start()

    loads[0].wait()
    loads[1].wait()
    own = g * leaves
    lanes = mass_v.shape[1]
    per = width // lanes
    for l in range(leaves):
        at = slice(l * width, (l + 1) * width)
        mass = jnp.concatenate([mass_v[per * l + k : per * l + k + 1, :] for k in range(per)], axis=1)
        w0, w1 = packed(pos_v[0:1, at], pos_v[1:2, at], pos_v[2:3, at], mass)
        table[own + l, 0:1, :] = w0
        table[own + l, 1:2, :] = w1
    loads[2].wait()
    pl.semaphore_wait(barrier, len(peers))

    halo = [
        pltpu.make_async_remote_copy(
            src_ref=mp_v.at[1], dst_ref=mp_v.at[1 - d], send_sem=halo_send.at[n], recv_sem=halo_recv.at[n],
            device_id={"zone": zone_at(d)}, device_id_type=MESH)
        for n, d in enumerate((1, -1))
    ]

    def block(o, dx=0):
        return table.at[pl.ds(grp_at(-o, dx) * leaves, leaves)]

    def z_copy(o, d):
        n = (o + d) % Z
        return pltpu.make_async_remote_copy(
            src_ref=block(o), dst_ref=block(o), send_sem=z_send.at[n], recv_sem=z_recv.at[n],
            device_id={"grp": grp_at(d, 0)}, device_id_type=MESH)

    def x_copy(o, dx):
        n = (dx - 1) * Z + o % Z
        return pltpu.make_async_remote_copy(
            src_ref=block(o), dst_ref=block(o), send_sem=x_send.at[n], recv_sem=x_recv.at[n],
            device_id={"grp": grp_at(0, dx)}, device_id_type=MESH)

    def x_onward(o, dx):
        n = Z + o % Z
        return pltpu.make_async_remote_copy(
            src_ref=block(o, -dx), dst_ref=block(o, -dx), send_sem=x_send.at[n], recv_sem=x_recv.at[n],
            device_id={"grp": grp_at(0, dx)}, device_id_type=MESH)

    def z_wait(o):
        n = o % Z
        pltpu.make_async_remote_copy(
            src_ref=block(o), dst_ref=block(o), send_sem=z_send.at[n], recv_sem=z_recv.at[n],
            device_id={"grp": grp_at(1, 0)}, device_id_type=MESH).wait_recv()

    def x_wait(o, dx):
        n = (dx - 1) * Z + o % Z
        pltpu.make_async_remote_copy(
            src_ref=block(o, -dx), dst_ref=block(o, -dx), send_sem=x_send.at[n], recv_sem=x_recv.at[n],
            device_id={"grp": grp_at(0, dx)}, device_id_type=MESH).wait_recv()

    sent = []
    near_dx = (1, X - 1)

    def send(make, *at):
        make(*at).start()
        sent.append((make, at))

    for h in halo:
        h.start()
    for d in reversed(reach):
        send(z_copy, 0, d)
    for dx in near_dx if 0 in RELAYS else range(1, X):
        send(x_copy, 0, dx)

    def x_relay(o):
        dx = near_dx[o % 2]
        x_wait(o, dx)
        send(x_onward, o, dx)

    def arrived(o):
        z_wait(o)
        if o % R == 0:
            sign, most = (1, plus) if o > 0 else (-1, minus)
            for d in range(min(R, most - abs(o)), 0, -1):
                send(z_copy, o, sign * d)
        for dx in near_dx[::-1]:
            if dx == 1 and abs(o) not in RELAYS:
                send(x_copy, o, 2)
            send(x_copy, o, dx)

    order = [o for r in range(1, plus + 1) for o in (r, -r) if o <= plus and -o <= minus]
    events = {}
    for o in sorted(order, key=lambda o: o % R != 0):
        events.setdefault(EVENTS.get(abs(o), "end"), []).append((arrived, o))
    for o in [0] + order:
        if abs(o) in RELAYS:
            events.setdefault(RELAYS[abs(o)], []).append((x_relay, o))

    def run_events(key):
        for act, o in events.get(key, ()):
            act(o)

    loads[3].wait()
    loads[4].wait()
    src_s[...] = jnp.full(src_s.shape, -1, I32)
    cls_s[...] = jnp.full(cls_s.shape, -1, I32)
    src_s[:, 0:far] = src_v[...]
    cls_s[:, 0:far] = place(cls_v[...])
    mp_s[...] = jnp.zeros(mp_s.shape, F32)

    def target_features(t, carry):
        tgt, px, py, pz = target_rows(*words(table, own + t, width))
        t_s[t] = jnp.transpose(tgt).astype(BF16)
        p_s[t] = jnp.concatenate([px, py, pz], axis=0)
        return carry

    lax.fori_loop(0, leaves, target_features, 0, unroll=True)
    for h in halo:
        h.wait_recv()
    keep = [(zone > 0).astype(F32), 1.0, (zone < zones - 1).astype(F32)]
    for d in range(3):
        mp_s[d * cells : (d + 1) * cells, 0:coeffs] = mp_v[d].astype(F32) * keep[d]
    mp = jnp.transpose(mp_s[...]).astype(BF16)
    nsrc = 3 * cells

    def gather_cells(i, carry):
        for u in range(UR):
            t = i * UR + u
            src = src_s[pl.ds(t, 1), :]
            pick = (lax.broadcasted_iota(I32, (nsrc, kpad), 0) == src).astype(F32).astype(BF16)
            r_s[t] = dot(mp, pick).astype(BF16)
        return carry

    lax.fori_loop(0, cells // UR, gather_cells, 0)
    run_events("r")

    def one_cell(t):
        cls = cls_s[pl.ds(t, 1), :]
        hot = (lax.broadcasted_iota(I32, (cpad, kpad), 0) == cls).astype(F32).astype(BF16)
        g = dot(hot, r_s[t], NT)
        for v in range(cpad // 8):
            part = g[8 * v : 8 * v + 8]
            shift, stride = (64 * (v // 8) + v % 8) * coeffs % 128, 8 * coeffs % 128
            if shift + 7 * stride >= 128:
                part = pltpu.roll(part, shift, 1)
                shift = 0
            part = pltpu.roll(part, shift, 1, stride=stride, stride_axis=0)
            g_s[pl.ds(pl.multiple_of(t * cpad + 8 * v, 8), 8), :] = part

    def some_cells(i, carry):
        for u in range(UG):
            one_cell(i * UG + u)
        for k in range(cells // UG):
            if ("g", k) in events:
                @pl.when(i == k)
                def _():
                    run_events(("g", k))
        return carry

    lax.fori_loop(0, cells // UG, some_cells, 0)
    lane = lax.broadcasted_iota(I32, (cells, 128), 1)
    tiles = (coeffs * classes + 127) // 128
    loads[7].wait()

    def rows_of(c):
        return g_s[pl.ds(place(c), cells, stride=cpad), :]

    def values(q):
        c = q * 128 // coeffs
        v = rows_of(c)
        while (c + 1) * coeffs < min(q * 128 + 128, coeffs * classes):
            c += 1
            v = jnp.where(lane < c * coeffs - q * 128, v, rows_of(c))
        if (c + 1) * coeffs < q * 128 + 128:
            v = jnp.where(lane < (c + 1) * coeffs - q * 128, v, 0.0)
        return v.astype(BF16)

    acc = jnp.zeros((cells, coeffs), F32)
    for q in range(0, tiles, 2):
        run_events(("f", q // 2))
        end = min(q * 128 + 256, coeffs * classes)
        o = ops_v[:, q * 128 : end]
        if end < q * 128 + 256:
            o = jnp.concatenate([o[:, :128], o[:, 128:], jnp.zeros((coeffs, q * 128 + 256 - end), o.dtype)], axis=1)
        acc = acc + dot(jnp.concatenate([values(q), values(q + 1)], axis=1), o, NT)
    loc_o[...] = acc
    run_events("end")

    loads[5].wait()
    loads[6].wait()
    for o in [0] + order:
        for dx in range(1, X):
            if not (abs(o) in RELAYS and dx == near_dx[o % 2]):
                x_wait(o, dx)

    def source_features(i, carry):
        for u in range(US):
            n = i * US + u
            rows, b = source_rows(*words(table, idx_s[n // near, n % near], width))
            s_s[n] = rows
            b_s[n] = b
        return carry

    lax.fori_loop(0, leaves * near // US, source_features, 0)

    def some_leaves(i, carry):
        for u in range(UL):
            t = i * UL + u
            acc = jnp.zeros((width, 8), F32)
            for s in range(near):
                n = t * near + s
                r = lax.rsqrt(dot(t_s[t], s_s[n]))
                acc = acc + dot((r * r * r).astype(BF16), b_s[n], NT)
            f_s[t] = acc
        return carry

    lax.fori_loop(0, leaves // UL, some_leaves, 0)
    for t in range(leaves):
        f = jnp.transpose(f_s[t])
        f = f[0:4] + f[4:8]
        on = jnp.concatenate([act_v[per * t + k : per * t + k + 1, :] for k in range(per)], axis=1).astype(F32)
        acc_o[:, t * width : (t + 1) * width] = (f[0:3] - p_s[t] * f[3:4]) * on
    for make, at in sent:
        make(*at).wait_send()
    for h in halo:
        h.wait_send()


UR, UG, US, UL = 16, 8, 8, 4
EVENTS = {1: ("g", 0), 2: ("g", 0), 3: ("g", 0), 4: ("f", 45), 5: ("f", 45), 6: ("f", 45)}
RELAYS = {}
MESH = pl.DeviceIdType.MESH
X_CHIPS = 4
REACH = 3


def on_device(positions, masses, active, near_src, multipoles, far_src, far_class, m2l_ops):
    leaves, near = near_src.shape
    particles = positions.shape[1]
    width = particles // leaves
    cells, far = far_src.shape
    coeffs = multipoles.shape[0]
    classes = m2l_ops.shape[1] // coeffs
    cpad = (classes + 63) // 64 * 64
    kpad = (far + 127) // 128 * 128
    zones, groups = lax.axis_size("zone"), lax.axis_size("grp")
    Z = groups // X_CHIPS
    cfg = (leaves, near, width, cells, far, coeffs, classes, cpad, kpad, zones, X_CHIPS, Z, REACH)
    accel, local = pl.pallas_call(
        functools.partial(kernel, cfg),
        out_shape=(jax.ShapeDtypeStruct((3, particles), F32), jax.ShapeDtypeStruct((cells, coeffs), F32)),
        in_specs=[pl.BlockSpec(memory_space=pl.ANY)] * 8,
        out_specs=(pl.BlockSpec(memory_space=pltpu.VMEM),) * 2,
        scratch_shapes=[
            pltpu.VMEM((3, particles), F32),
            pltpu.VMEM((particles // 128, 128), F32),
            pltpu.VMEM((particles // 128, 128), I32),
            pltpu.SMEM((leaves, near), I32),
            pltpu.VMEM((3, cells, coeffs), BF16),
            pltpu.VMEM((cells, far), I32),
            pltpu.VMEM((cells, far), I32),
            pltpu.VMEM(m2l_ops.shape, BF16),
            pltpu.VMEM((groups * leaves, 2, width), I32),
            pltpu.VMEM((cells, kpad), I32),
            pltpu.VMEM((cells, kpad), I32),
            pltpu.VMEM((3 * cells, 128), F32),
            pltpu.VMEM((cells, 128, kpad), BF16),
            pltpu.VMEM((cpad * cells, 128), F32),
            pltpu.VMEM((leaves, width, 32), BF16),
            pltpu.VMEM((leaves, 3, width), F32),
            pltpu.VMEM((leaves * near, 32, width), BF16),
            pltpu.VMEM((leaves * near, 8, width), BF16),
            pltpu.VMEM((leaves, width, 8), F32),
            pltpu.SemaphoreType.DMA((8,)),
            pltpu.SemaphoreType.DMA((2,)),
            pltpu.SemaphoreType.DMA((2,)),
            pltpu.SemaphoreType.DMA((Z,)),
            pltpu.SemaphoreType.DMA((Z,)),
            pltpu.SemaphoreType.DMA(((X_CHIPS - 1) * Z,)),
            pltpu.SemaphoreType.DMA(((X_CHIPS - 1) * Z,)),
        ],
        compiler_params=pltpu.CompilerParams(
            collective_id=0, has_side_effects=True, vmem_limit_bytes=67043328),
    )(positions, masses.reshape(-1, 128), active.reshape(-1, 128), near_src, multipoles.T, far_src, far_class, m2l_ops)
    accel, local = pl.pallas_call(
        hand_over,
        out_shape=(jax.ShapeDtypeStruct(accel.shape, F32), jax.ShapeDtypeStruct(local.shape, F32)),
        in_specs=[pl.BlockSpec(memory_space=pl.ANY)] * 2,
        out_specs=(pl.BlockSpec(memory_space=pl.ANY),) * 2,
        scratch_shapes=[pltpu.VMEM(accel.shape, F32), pltpu.VMEM(local.shape, F32), pltpu.SemaphoreType.DMA((4,))],
    )(accel, local)
    return accel, local.T


def hand_over(a_in, b_in, a_out, b_out, a_v, b_v, sem):
    copies = [
        pltpu.make_async_copy(x, y, sem.at[n])
        for n, (x, y) in enumerate([(a_in, a_v), (b_in, b_v), (a_v, a_out), (b_v, b_out)])
    ]
    copies[0].start()
    copies[1].start()
    copies[1].wait()
    copies[3].start()
    copies[0].wait()
    copies[2].start()
    copies[2].wait()
    copies[3].wait()


def solution(mesh):
    return jax.shard_map(
        on_device,
        mesh=mesh,
        in_specs=(
            P(None, ("zone", "grp")),
            P(("zone", "grp")),
            P(("zone", "grp")),
            P(("zone", "grp"), None),
            P(None, ("zone", "grp")),
            P(("zone", "grp"), None),
            P(("zone", "grp"), None),
            P(),
        ),
        out_specs=(P(None, ("zone", "grp")), P(None, ("zone", "grp"))),
        check_vma=False,
    )
```
